32 devices in a mesh: rep: 1, dp: 32 (over x, y, z, core).
Axes of the slice: x: 2, y: 2, z: 4, core: 2. Of those that a mesh axis runs over, the one named last changes fastest.
Arguments:
- x: bfloat16 [32, 2048, 1024], P(('rep', 'dp'))
- dy: bfloat16 [32, 2048, 1024], P(('rep', 'dp'))
- w_gate: bfloat16 [2, 1024, 3200], replicated
- w_up: bfloat16 [2, 1024, 3200], replicated
- w_down: bfloat16 [2, 3200, 1024], replicated
- m_w_gate: float32 [2, 1024, 3200], P(None, 'dp')
- m_w_up: float32 [2, 1024, 3200], P(None, 'dp')
- m_w_down: float32 [2, 3200, 1024], P(None, 'dp')
- v_w_gate: float32 [2, 1024, 3200], P(None, 'dp')
- v_w_up: float32 [2, 1024, 3200], P(None, 'dp')
- v_w_down: float32 [2, 3200, 1024], P(None, 'dp')
Outputs:
- output 1: bfloat16 [2, 1024, 3200], P('rep')
- output 2: bfloat16 [2, 1024, 3200], P('rep')
- output 3: bfloat16 [2, 3200, 1024], P('rep')
- output 4: float32 [2, 1024, 3200], P('rep', 'dp')
- output 5: float32 [2, 1024, 3200], P('rep', 'dp')
- output 6: float32 [2, 3200, 1024], P('rep', 'dp')
- output 7: float32 [2, 1024, 3200], P('rep', 'dp')
- output 8: float32 [2, 1024, 3200], P('rep', 'dp')
- output 9: float32 [2, 3200, 1024], P('rep', 'dp')
All inputs are finite; a program needn't handle non-finite values.
Results may differ from the reference program's by a relative error of at most 0.022.
Values are sent between devices in bfloat16 or wider.
A program may use at most 2 GiB of HBM per device.

```python
import jax
import jax.numpy as jnp
from jax import lax

SEQUENCES = 32
TOKENS = 2048
D = 1024
FF = 3200
LAYERS = 2
NAMES = ("w_gate", "w_up", "w_down")
SHAPES = {"w_gate": (LAYERS, D, FF), "w_up": (LAYERS, D, FF), "w_down": (LAYERS, FF, D)}


def bump(key, n, height):
    away = (jnp.arange(n, dtype=jnp.int32) - jax.random.randint(key, (), 0, n, jnp.int32)) % n
    return jnp.where(away < n // 8, height, 1.0)


def together(key, own, strength):
    shared = jax.random.normal(key, own.shape[1:], jnp.float32)
    return (own + strength * shared) * lax.rsqrt(1 + strength * strength)


def setup_inputs(seed: int = 0, part: int = 0) -> dict:
    kx, kdy, ka, kb, kz, kf, kh, kl, *keys = jax.random.split(jax.random.key(seed), 8 + 3 * len(NAMES))
    kx, kdy, ka, kb = (jax.random.fold_in(k, part) for k in (kx, kdy, ka, kb))
    kw, km, kv = (keys[i::3] for i in range(3))
    shape = (SEQUENCES, TOKENS, D)
    much_x, much_dy = jax.random.uniform(kz, (2,), jnp.float32, 0.0, 1.0)
    loud = 2.0 ** jax.random.uniform(jax.random.fold_in(kz, 1), (), jnp.float32, -1.0, 2.0)
    layers = 2.0 ** jax.random.uniform(kl, (LAYERS, 1, 1), jnp.float32, -1.0, 1.0)
    x = together(ka, jax.random.normal(kx, shape, jnp.float32), much_x) * bump(kf, D, 4.0)
    dy = together(kb, jax.random.normal(kdy, shape, jnp.float32), much_dy)
    drawn = {"x": x.astype(jnp.bfloat16), "dy": (loud * dy * (SEQUENCES * TOKENS) ** -0.5).astype(jnp.bfloat16)}
    for key, name in zip(kw, NAMES, strict=True):
        w = jax.random.normal(key, SHAPES[name], jnp.float32) * SHAPES[name][1] ** -0.5
        drawn[name] = (w * {"w_gate": 1.0, "w_up": bump(kh, FF, 4.0), "w_down": layers}[name]).astype(jnp.bfloat16)
    for key, name in zip(km, NAMES, strict=True):
        drawn[f"m_{name}"] = 0.1 * jax.random.normal(key, SHAPES[name], jnp.float32)
    for key, name in zip(kv, NAMES, strict=True):
        drawn[f"v_{name}"] = jax.random.uniform(key, SHAPES[name], jnp.float32, 0.005, 0.015)
    return drawn


def matmul(a, w):
    return jnp.dot(a, w, preferred_element_type=jnp.float32).astype(jnp.bfloat16)


def normed(h):
    wide = h.astype(jnp.float32)
    scale = lax.rsqrt(jnp.mean(wide**2, -1, keepdims=True) + 1e-6)
    return (wide * scale).astype(jnp.bfloat16)


def layer(h, w):
    a = normed(h)
    gate = jnp.dot(a, w["w_gate"], preferred_element_type=jnp.float32)
    up = jnp.dot(a, w["w_up"], preferred_element_type=jnp.float32)
    return h + matmul((jax.nn.silu(gate) * up).astype(jnp.bfloat16), w["w_down"])


def adamw(w, m, v, g):
    m = 0.9 * m + 0.1 * g
    v = 0.95 * v + 0.05 * g * g
    step = m * lax.rsqrt(v + 1e-8) + 0.1 * w
    return (w - 0.02 * step).astype(jnp.bfloat16), m, v


def stack(weights, h):
    return lax.scan(lambda h, w: (layer(h, w), None), h, weights)[0]


def reference(x, dy, w_gate, w_up, w_down, m_w_gate, m_w_up, m_w_down, v_w_gate, v_w_up, v_w_down):
    weights = dict(zip(NAMES, (w_gate, w_up, w_down), strict=True))

    def take(so_far, sequence):
        h, by_y = sequence
        _, back = jax.vjp(lambda w: stack(w, h), weights)
        return jax.tree.map(lambda total, term: total + term.astype(jnp.float32), so_far, back(by_y)[0]), None

    none_yet = {name: jnp.zeros(w.shape, jnp.float32) for name, w in weights.items()}
    by_weights, _ = lax.scan(take, none_yet, (x, dy))
    gradients = [by_weights[name].astype(jnp.bfloat16).astype(jnp.float32) for name in NAMES]
    new = [
        adamw(w.astype(jnp.float32), m, v, g)
        for w, m, v, g in zip((w_gate, w_up, w_down), (m_w_gate, m_w_up, m_w_down), (v_w_gate, v_w_up, v_w_down), gradients, strict=True)
    ]
    return tuple(one[which] for which in range(3) for one in new)
```

```python
import functools

import jax
import jax.numpy as jnp
from jax import lax
from jax.experimental import pallas as pl
from jax.experimental.pallas import tpu as pltpu
from jax.sharding import PartitionSpec as P

F32 = jnp.float32
BF16 = jnp.bfloat16
MESH = pl.DeviceIdType.MESH
WEIGHT = (16, 8, 4, 2, 1)
X, Y, Z1, Z0, CORE = range(5)
ORDERS = ((X, Y, Z0, Z1), (Y, X, Z0, Z1), (Z0, Z1, X, Y))
COLUMNS = ((0, 1280), (1280, 1280), (2560, 640))
ROWS = ((0, 80), (80, 80), (160, 40))
ROWWISE, COLWISE = (32, 3200), (200, 512)
KINDS = ("d", "g", "u")


def dot(a, b, ca, cb):
    return lax.dot_general(a, b, (((ca,), (cb,)), ((), ())), preferred_element_type=F32)


def norm(h):
    wide = h.astype(F32)
    scale = lax.rsqrt(jnp.mean(wide**2, -1, keepdims=True) + 1e-6)
    return (wide * scale).astype(BF16), scale


def adamw(w, m, v, g):
    m = 0.9 * m + 0.1 * g
    v = 0.95 * v + 0.05 * g * g
    step = m * lax.rsqrt(v + 1e-8) + 0.1 * w
    return (w - 0.02 * step).astype(BF16), m, v


def half_of(kind):
    return COLWISE if kind == "d" else ROWWISE


def part_of(kind, color):
    rows, columns = half_of(kind)
    if kind == "d":
        at, n = ROWS[color]
        return (pl.ds(at, n), slice(None)), (n, columns)
    at, n = COLUMNS[color]
    return (slice(None), pl.ds(at, n)), (rows, n)


def place():
    me = lax.axis_index("dp")
    bits = tuple(lax.rem(lax.div(me, w), 2) for w in WEIGHT)
    partners = tuple(me + (1 - 2 * b) * w for b, w in zip(bits, WEIGHT))
    return bits, partners


def greet(partners):
    barrier = pltpu.get_barrier_semaphore()
    for p in partners:
        pl.semaphore_signal(barrier, inc=1, device_id={"dp": p}, device_id_type=MESH)
    pl.semaphore_wait(barrier, len(partners))


def remote(src, dst, send, recv, to):
    return pltpu.make_async_remote_copy(src_ref=src, dst_ref=dst, send_sem=send, recv_sem=recv, device_id={"dp": to}, device_id_type=MESH)


def free_of(index):
    return [i for i in range(4) if index[i] is None]


def for_blocks(index, body):
    free = free_of(index)

    def one(n, _):
        at = list(index)
        for k, i in enumerate(free):
            at[i] = lax.rem(lax.div(n, 2 ** (len(free) - 1 - k)), 2)
        body(tuple(at))
        return 0

    lax.fori_loop(0, 2 ** len(free), one, 0)


def window(index):
    return tuple(slice(None) if i is None else i for i in index)


def reduce_kernel(kinds, *refs):
    n = len(kinds)
    grads, outs, refs = refs[:n], refs[n : 2 * n], refs[2 * n :]
    totals, firsts, refs = refs[:n], refs[n : 2 * n], refs[2 * n :]
    gots, refs = [refs[12 * u : 12 * u + 12] for u in range(n)], refs[12 * n :]
    last, send, recv, local = refs
    bits, partners = place()
    core = bits[CORE]
    greet(partners)

    def halves(u, which):
        if kinds[u] == "d":
            return grads[u].at[:, :, :, :, :, pl.ds(pl.multiple_of(which * 512, 512), 512)]
        return grads[u].at[:, :, :, :, which]

    started = {}
    for u in range(n):
        copy = remote(halves(u, 1 - core), firsts[u], send.at[u, 12], recv.at[u, 12], partners[CORE])
        copy.start()
        own = pltpu.make_async_copy(halves(u, core), totals[u], local.at[u])
        own.start()
        started[u] = (copy, own)

    state = {(u, color): [None] * 4 for u in range(n) for color in range(3)}
    flying = {}

    def total(u, color, at, steps):
        where = (*at, *part_of(kinds[u], color)[0])
        value = totals[u][where].astype(F32) + firsts[u][where].astype(F32)
        for s in range(steps):
            rest = tuple(at[i] for i in range(4) if i not in ORDERS[color][: s + 1])
            got = gots[u][color * 4 + s]
            value += (got[rest] if rest else got[...]).astype(F32)
        return value.astype(BF16)

    def launch(u, color, s):
        dim = ORDERS[color][s]
        part, _ = part_of(kinds[u], color)
        index = list(state[u, color])
        index[dim] = 1 - bits[dim]
        k = color * 4 + s

        def ready(at):
            totals[u][(*at, *part)] = total(u, color, at, s)

        for_blocks(index, ready)
        copy = remote(totals[u].at[(*window(index), *part)], gots[u][k], send.at[u, k], recv.at[u, k], partners[dim])
        copy.start()
        flying[u, color] = copy
        index[dim] = bits[dim]
        state[u, color] = index

    waits = []
    for t in range(n + 4):
        for u in reversed(range(n)):
            s = t - u
            if s == 0:
                copy, own = started[u]
                own.wait()
                copy.wait_recv()
                waits.append(copy)
                for color in range(3):
                    launch(u, color, 0)
            elif 0 < s <= 4:
                for color in range(3):
                    copy = flying[u, color]
                    copy.wait_recv()
                    waits.append(copy)
                    if s < 4:
                        launch(u, color, s)
                        continue
                    (rows, columns), _ = part_of(kinds[u], color)
                    if kinds[u] == "d":
                        last[rows, pl.ds(pl.multiple_of(core * 512, 512), 512)] = total(u, color, bits[:4], 4)
                    else:
                        outs[u][rows, columns] = total(u, color, bits[:4], 4)
                if s == 4:
                    if kinds[u] == "d":
                        columns = (slice(None), pl.ds(pl.multiple_of(core * 512, 512), 512))
                        copy = remote(last.at[columns], last.at[columns], send.at[u, 13], recv.at[u, 13], partners[CORE])
                        copy.start()
                        flying["d"] = copy
    for u in range(n):
        if kinds[u] == "d":
            copy = flying["d"]
            copy.wait_recv()
            waits.append(copy)
            outs[u][...] = last[...]
    for copy in waits:
        copy.wait_send()


def reduce_scatter(grads, kinds, collective_id):
    n = len(kinds)
    blocks = lambda shape: pltpu.VMEM((2, 2, 2, 2, *shape), BF16)
    scratch = [blocks(half_of(k)) for k in kinds] * 2
    for k in kinds:
        for color in range(3):
            for s in range(4):
                scratch.append(pltpu.VMEM((2,) * (3 - s) + part_of(k, color)[1], BF16))
    scratch += [pltpu.VMEM((200, 1024), BF16), pltpu.SemaphoreType.DMA((n, 14)), pltpu.SemaphoreType.DMA((n, 14)), pltpu.SemaphoreType.DMA((n,))]
    return pl.pallas_call(
        functools.partial(reduce_kernel, kinds),
        out_shape=[jax.ShapeDtypeStruct((200, 1024) if k == "d" else (32, 3200), BF16) for k in kinds],
        in_specs=[pl.BlockSpec(memory_space=pltpu.HBM)] * n,
        out_specs=[pl.BlockSpec(memory_space=pltpu.VMEM)] * n,
        scratch_shapes=scratch,
        compiler_params=pltpu.CompilerParams(collective_id=collective_id, has_side_effects=True, vmem_limit_bytes=60 * 2**20),
        name=f"reduce_{collective_id}",
    )(*grads)


def gather_kernel(units, *refs):
    n = len(units)
    blocks, outs, (send, recv, local) = refs[:n], refs[n : n + 3], refs[n + 3 :]
    bits, partners = place()
    core = bits[CORE]
    greet(partners)

    def at(u, index, color):
        kind, layer = units[u]
        (rows, columns), _ = part_of(kind, color)
        out = outs[KINDS.index(kind)]
        if kind == "d":
            return out.at[(layer, *window(index), rows, pl.ds(pl.multiple_of(core * 512, 512), 512))]
        return out.at[(layer, *window(index), core, rows, columns)]

    sent = []
    flying = {}
    state = {}

    def across(u, color, src, index, k):
        dst = at(u, index, color)
        copy = remote(dst if src is None else src, dst, send.at[u, 9 * color + k], recv.at[u, 9 * color + k], partners[CORE])
        copy.start()
        sent.append((copy, True))

    def launch(u, color, s, src=None):
        dim = ORDERS[color][3 - s]
        dst = at(u, state[u, color], color)
        copy = remote(dst if src is None else src, dst, send.at[u, 9 * color + s], recv.at[u, 9 * color + s], partners[dim])
        copy.start()
        flying[u, color] = copy

    for t in range(n + 4):
        for u in reversed(range(n)):
            s = t - u
            if s == 0:
                kind, layer = units[u]
                for color in range(3):
                    state[u, color] = list(bits[:4])
                    (rows, columns), _ = part_of(kind, color)
                    src = blocks[u].at[rows, columns]
                    launch(u, color, 0, src)
                    across(u, color, src, state[u, color], 4)
                    own = pltpu.make_async_copy(src, at(u, state[u, color], color), local.at[u, color])
                    own.start()
                    flying["own", u, color] = own
            elif 0 < s <= 4:
                for color in range(3):
                    copy = flying[u, color]
                    copy.wait_recv()
                    sent.append((copy, False))
                    if s == 1:
                        flying["own", u, color].wait()
                    dim = ORDERS[color][4 - s]
                    fresh = list(state[u, color])
                    fresh[dim] = 1 - bits[dim]
                    state[u, color][dim] = None
                    if s < 4:
                        launch(u, color, s)
                    across(u, color, None, fresh, 4 + s)
    for copy, from_core in sent:
        copy.wait_send()
        if from_core:
            copy.wait_recv()


def all_gather(blocks, units, layers, collective_id):
    n = len(units)
    shapes = [(layers, 2, 2, 2, 2, 200, 1024)] + [(layers, 2, 2, 2, 2, 2, 32, 3200)] * 2
    return pl.pallas_call(
        functools.partial(gather_kernel, units),
        out_shape=[jax.ShapeDtypeStruct(s, BF16) for s in shapes],
        in_specs=[pl.BlockSpec(memory_space=pltpu.VMEM)] * n,
        out_specs=[pl.BlockSpec(memory_space=pltpu.HBM)] * 3,
        scratch_shapes=[pltpu.SemaphoreType.DMA((n, 27)), pltpu.SemaphoreType.DMA((n, 27)), pltpu.SemaphoreType.DMA((n, 3))],
        compiler_params=pltpu.CompilerParams(collective_id=collective_id, has_side_effects=True),
        name=f"gather_{collective_id}",
    )(*blocks)


def solution(mesh):
    def local(x, dy, wg, wu, wd, mg, mu, md, vg, vu, vd):
        x, dy = x[0], dy[0]
        me = lax.axis_index("dp")
        core = lax.rem(me, 2)
        layers = wg.shape[0]
        old = {"g": (wg, mg, vg), "u": (wu, mu, vu), "d": (wd, md, vd)}

        h = x
        saved = []
        for i in range(layers):
            a, scale = norm(h)
            gate = dot(a, wg[i], 1, 0)
            up = dot(a, wu[i], 1, 0)
            act = (jax.nn.silu(gate) * up).astype(BF16)
            saved.append((h, a, scale, gate, up, act))
            if i + 1 < layers:
                h = h + dot(act, wd[i], 1, 0).astype(BF16)
        d = dy
        summed = {}
        for i in reversed(range(layers)):
            h, a, scale, gate, up, act = saved[i]
            by_d = dot(act, d, 0, 0).astype(BF16)
            d_act = dot(d, wd[i], 1, 1).astype(BF16).astype(F32)
            sig = jax.nn.sigmoid(gate)
            d_up = (d_act * (gate * sig)).astype(BF16)
            d_gate = (d_act * up * (sig * (1 + gate * (1 - sig)))).astype(BF16)
            by_g = dot(a, d_gate, 0, 0).astype(BF16)
            by_u = dot(a, d_up, 0, 0).astype(BF16)
            grads = [by_d.reshape(2, 2, 2, 2, 200, 1024)] + [t.reshape(2, 2, 2, 2, 2, 32, 3200) for t in (by_g, by_u)]
            summed[i] = dict(zip(KINDS, reduce_scatter(grads, KINDS, i)))
            if i:
                da = dot(d_gate, wg[i], 1, 1).astype(BF16) + dot(d_up, wu[i], 1, 1).astype(BF16)
                da = da.astype(F32)
                wide = h.astype(F32)
                inner = jnp.mean(da * wide, -1, keepdims=True)
                d = d + (scale * da - wide * (scale**3 * inner)).astype(BF16)
        new = {}
        for kind in KINDS:
            w, m, v = old[kind]
            rows = m.shape[1]
            g = jnp.stack([summed[i][kind] for i in range(layers)])
            if kind == "d":
                g = lax.dynamic_slice_in_dim(g, core * rows, rows, 1)
            mine = lax.dynamic_slice_in_dim(w, me * rows, rows, 1)
            new[kind] = adamw(mine.astype(F32), m, v, g.astype(F32))
        mine = new["d"][0]
        other = lax.ppermute(mine, "dp", [(k, k + 1 - 2 * (k % 2)) for k in range(32)])
        first = core == 0
        whole = jnp.concatenate([jnp.where(first, mine, other), jnp.where(first, other, mine)], 1)
        part = {"d": lax.dynamic_slice_in_dim(whole, core * 512, 512, 2), "g": new["g"][0], "u": new["u"][0]}
        units = tuple((kind, i) for i in reversed(range(layers)) for kind in KINDS)
        full = all_gather([part[kind][i] for kind, i in units], units, layers, 2)
        full = {kind: t.reshape(old[kind][0].shape) for kind, t in zip(KINDS, full)}
        return tuple(full[k] for k in "gud") + tuple(new[k][1] for k in "gud") + tuple(new[k][2] for k in "gud")

    seq, whole, rows = P(("rep", "dp")), P(), P(None, "dp")
    return jax.shard_map(
        local,
        mesh=mesh,
        in_specs=(seq, seq, whole, whole, whole) + (rows,) * 6,
        out_specs=(P("rep"),) * 3 + (P("rep", "dp"),) * 6,
        check_vma=False,
    )
```

```python
import functools

import jax
import jax.numpy as jnp
from jax import lax
from jax.experimental import pallas as pl
from jax.experimental.pallas import tpu as pltpu
from jax.sharding import PartitionSpec as P

F32 = jnp.float32
BF16 = jnp.bfloat16
MESH = pl.DeviceIdType.MESH
WEIGHT = (16, 8, 4, 2, 1)
X, Y, Z1, Z0, CORE = range(5)
ORDERS = ((X, Y, Z0, Z1), (Y, X, Z0, Z1), (Z0, Z1, X, Y))
COLUMNS = ((0, 1280), (1280, 1280), (2560, 640))
ROWS = ((0, 80), (80, 80), (160, 40))
ROWWISE, COLWISE = (32, 3200), (200, 512)
KINDS = ("d", "g", "u")


def dot(a, b, ca, cb):
    return lax.dot_general(a, b, (((ca,), (cb,)), ((), ())), preferred_element_type=F32)


def norm(h):
    wide = h.astype(F32)
    scale = lax.rsqrt(jnp.mean(wide**2, -1, keepdims=True) + 1e-6)
    return (wide * scale).astype(BF16), scale


def adamw(w, m, v, g):
    m = 0.9 * m + 0.1 * g
    v = 0.95 * v + 0.05 * g * g
    step = m * lax.rsqrt(v + 1e-8) + 0.1 * w
    return (w - 0.02 * step).astype(BF16), m, v


def half_of(kind):
    return COLWISE if kind == "d" else ROWWISE


def part_of(kind, color):
    rows, columns = half_of(kind)
    if kind == "d":
        at, n = ROWS[color]
        return (pl.ds(at, n), slice(None)), (n, columns)
    at, n = COLUMNS[color]
    return (slice(None), pl.ds(at, n)), (rows, n)


def place():
    me = lax.axis_index("dp")
    bits = tuple(lax.rem(lax.div(me, w), 2) for w in WEIGHT)
    partners = tuple(me + (1 - 2 * b) * w for b, w in zip(bits, WEIGHT))
    return bits, partners


def greet(partners):
    barrier = pltpu.get_barrier_semaphore()
    for p in partners:
        pl.semaphore_signal(barrier, inc=1, device_id={"dp": p}, device_id_type=MESH)
    pl.semaphore_wait(barrier, len(partners))


def remote(src, dst, send, recv, to):
    return pltpu.make_async_remote_copy(src_ref=src, dst_ref=dst, send_sem=send, recv_sem=recv, device_id={"dp": to}, device_id_type=MESH)


def free_of(index):
    return [i for i in range(4) if index[i] is None]


def for_blocks(index, body):
    free = free_of(index)

    def one(n, _):
        at = list(index)
        for k, i in enumerate(free):
            at[i] = lax.rem(lax.div(n, 2 ** (len(free) - 1 - k)), 2)
        body(tuple(at))
        return 0

    lax.fori_loop(0, 2 ** len(free), one, 0)


def window(index):
    return tuple(slice(None) if i is None else i for i in index)


def reduce_kernel(kinds, *refs):
    n = len(kinds)
    grads, outs, refs = refs[:n], refs[n : 2 * n], refs[2 * n :]
    totals, firsts, refs = refs[:n], refs[n : 2 * n], refs[2 * n :]
    gots, refs = [refs[12 * u : 12 * u + 12] for u in range(n)], refs[12 * n :]
    lasts = {}
    for u in range(n):
        if kinds[u] == "d":
            lasts[u], refs = refs[0], refs[1:]
    send, recv, local = refs
    bits, partners = place()
    core = bits[CORE]
    greet(partners)

    def halves(u, which):
        if kinds[u] == "d":
            return grads[u].at[:, :, :, :, :, pl.ds(pl.multiple_of(which * 512, 512), 512)]
        return grads[u].at[:, :, :, :, which]

    started = {}
    for u in range(n):
        copy = remote(halves(u, 1 - core), firsts[u], send.at[u, 12], recv.at[u, 12], partners[CORE])
        copy.start()
        own = pltpu.make_async_copy(halves(u, core), totals[u], local.at[u])
        own.start()
        started[u] = (copy, own)

    state = {(u, color): [None] * 4 for u in range(n) for color in range(3)}
    flying = {}

    def total(u, color, at, steps):
        where = (*at, *part_of(kinds[u], color)[0])
        value = totals[u][where].astype(F32) + firsts[u][where].astype(F32)
        for s in range(steps):
            rest = tuple(at[i] for i in range(4) if i not in ORDERS[color][: s + 1])
            got = gots[u][color * 4 + s]
            value += (got[rest] if rest else got[...]).astype(F32)
        return value.astype(BF16)

    def launch(u, color, s):
        dim = ORDERS[color][s]
        part, _ = part_of(kinds[u], color)
        index = list(state[u, color])
        index[dim] = 1 - bits[dim]
        k = color * 4 + s

        def ready(at):
            totals[u][(*at, *part)] = total(u, color, at, s)

        for_blocks(index, ready)
        copy = remote(totals[u].at[(*window(index), *part)], gots[u][k], send.at[u, k], recv.at[u, k], partners[dim])
        copy.start()
        flying[u, color] = copy
        index[dim] = bits[dim]
        state[u, color] = index

    waits = []
    for t in range(n + 4):
        for u in reversed(range(n)):
            s = t - u
            if s == 0:
                copy, own = started[u]
                own.wait()
                copy.wait_recv()
                waits.append(copy)
                for color in range(3):
                    launch(u, color, 0)
            elif 0 < s <= 4:
                for color in range(3):
                    copy = flying[u, color]
                    copy.wait_recv()
                    waits.append(copy)
                    if s < 4:
                        launch(u, color, s)
                        continue
                    (rows, columns), _ = part_of(kinds[u], color)
                    if kinds[u] == "d":
                        lasts[u][rows, pl.ds(pl.multiple_of(core * 512, 512), 512)] = total(u, color, bits[:4], 4)
                    else:
                        outs[u][rows, columns] = total(u, color, bits[:4], 4)
                if s == 4:
                    if kinds[u] == "d":
                        columns = (slice(None), pl.ds(pl.multiple_of(core * 512, 512), 512))
                        copy = remote(lasts[u].at[columns], lasts[u].at[columns], send.at[u, 13], recv.at[u, 13], partners[CORE])
                        copy.start()
                        flying["d", u] = copy
    for u in range(n):
        if kinds[u] == "d":
            copy = flying["d", u]
            copy.wait_recv()
            waits.append(copy)
            outs[u][...] = lasts[u][...]
    for copy in waits:
        copy.wait_send()


def reduce_scatter(grads, kinds, collective_id):
    n = len(kinds)
    blocks = lambda shape: pltpu.VMEM((2, 2, 2, 2, *shape), BF16)
    scratch = [blocks(half_of(k)) for k in kinds] * 2
    for k in kinds:
        for color in range(3):
            for s in range(4):
                scratch.append(pltpu.VMEM((2,) * (3 - s) + part_of(k, color)[1], BF16))
    scratch += [pltpu.VMEM((200, 1024), BF16)] * kinds.count("d")
    scratch += [pltpu.SemaphoreType.DMA((n, 14)), pltpu.SemaphoreType.DMA((n, 14)), pltpu.SemaphoreType.DMA((n,))]
    return pl.pallas_call(
        functools.partial(reduce_kernel, kinds),
        out_shape=[jax.ShapeDtypeStruct((200, 1024) if k == "d" else (32, 3200), BF16) for k in kinds],
        in_specs=[pl.BlockSpec(memory_space=pltpu.HBM)] * n,
        out_specs=[pl.BlockSpec(memory_space=pltpu.VMEM)] * n,
        scratch_shapes=scratch,
        compiler_params=pltpu.CompilerParams(collective_id=collective_id, has_side_effects=True, vmem_limit_bytes=62 * 2**20),
        name=f"reduce_{collective_id}",
    )(*grads)


def gather_kernel(kinds, *refs):
    n = len(kinds)
    blocks, outs, (send, recv, local) = refs[:n], refs[n : 2 * n], refs[2 * n :]
    bits, partners = place()
    core = bits[CORE]
    greet(partners)

    def at(u, index, color):
        (rows, columns), _ = part_of(kinds[u], color)
        out = outs[u]
        if kinds[u] == "d":
            return out.at[(*window(index), rows, pl.ds(pl.multiple_of(core * 512, 512), 512))]
        return out.at[(*window(index), core, rows, columns)]

    sent = []
    flying = {}
    state = {}

    def across(u, color, src, index, k):
        dst = at(u, index, color)
        copy = remote(dst if src is None else src, dst, send.at[u, 9 * color + k], recv.at[u, 9 * color + k], partners[CORE])
        copy.start()
        sent.append((copy, True))

    def launch(u, color, s, src=None):
        dim = ORDERS[color][3 - s]
        dst = at(u, state[u, color], color)
        copy = remote(dst if src is None else src, dst, send.at[u, 9 * color + s], recv.at[u, 9 * color + s], partners[dim])
        copy.start()
        flying[u, color] = copy

    for t in range(n + 4):
        for u in reversed(range(n)):
            s = t - u
            if s == 0:
                for color in range(3):
                    state[u, color] = list(bits[:4])
                    (rows, columns), _ = part_of(kinds[u], color)
                    src = blocks[u].at[rows, columns]
                    launch(u, color, 0, src)
                    across(u, color, src, state[u, color], 4)
                    own = pltpu.make_async_copy(src, at(u, state[u, color], color), local.at[u, color])
                    own.start()
                    flying["own", u, color] = own
            elif 0 < s <= 4:
                for color in range(3):
                    copy = flying[u, color]
                    copy.wait_recv()
                    sent.append((copy, False))
                    if s == 1:
                        flying["own", u, color].wait()
                    dim = ORDERS[color][4 - s]
                    fresh = list(state[u, color])
                    fresh[dim] = 1 - bits[dim]
                    state[u, color][dim] = None
                    if s < 4:
                        launch(u, color, s)
                    across(u, color, None, fresh, 4 + s)
    for copy, from_core in sent:
        copy.wait_send()
        if from_core:
            copy.wait_recv()


def all_gather(blocks, kinds, collective_id):
    n = len(kinds)
    shapes = [(2, 2, 2, 2, 200, 1024) if k == "d" else (2, 2, 2, 2, 2, 32, 3200) for k in kinds]
    return pl.pallas_call(
        functools.partial(gather_kernel, kinds),
        out_shape=[jax.ShapeDtypeStruct(s, BF16) for s in shapes],
        in_specs=[pl.BlockSpec(memory_space=pltpu.VMEM)] * n,
        out_specs=[pl.BlockSpec(memory_space=pltpu.HBM)] * n,
        scratch_shapes=[pltpu.SemaphoreType.DMA((n, 27)), pltpu.SemaphoreType.DMA((n, 27)), pltpu.SemaphoreType.DMA((n, 3))],
        compiler_params=pltpu.CompilerParams(collective_id=collective_id, has_side_effects=True),
        name=f"gather_{collective_id}",
    )(*blocks)


def solution(mesh):
    def local(x, dy, wg, wu, wd, mg, mu, md, vg, vu, vd):
        x, dy = x[0], dy[0]
        me = lax.axis_index("dp")
        core = lax.rem(me, 2)
        layers = wg.shape[0]
        old = {"g": (wg, mg, vg), "u": (wu, mu, vu), "d": (wd, md, vd)}

        h = x
        saved = []
        for i in range(layers):
            a, scale = norm(h)
            gate = dot(a, wg[i], 1, 0)
            up = dot(a, wu[i], 1, 0)
            act = (jax.nn.silu(gate) * up).astype(BF16)
            saved.append((h, a, scale, gate, up, act))
            if i + 1 < layers:
                h = h + dot(act, wd[i], 1, 0).astype(BF16)
        def rows_of(t, kind):
            rows = old[kind][1].shape[1]
            return lax.dynamic_slice_in_dim(t, me * rows, rows, 0)

        def update(kind, i, g):
            w, m, v = (t[i] for t in old[kind])
            return adamw(rows_of(w, kind).astype(F32), m, v, g.astype(F32))

        def by_chips(t, kind):
            return t.reshape(2, 2, 2, 2, 200, 1024) if kind == "d" else t.reshape(2, 2, 2, 2, 2, 32, 3200)

        d = dy
        grads, new, full = {}, {}, {}
        for i in reversed(range(layers)):
            h, a, scale, gate, up, act = saved[i]
            d_act = dot(d, wd[i], 1, 1).astype(BF16).astype(F32)
            sig = jax.nn.sigmoid(gate)
            d_up = (d_act * (gate * sig)).astype(BF16)
            d_gate = (d_act * up * (sig * (1 + gate * (1 - sig)))).astype(BF16)
            grads["g", i] = dot(a, d_gate, 0, 0).astype(BF16)
            if i:
                early = lax.psum_scatter(grads.pop(("g", i)).reshape(32, 32, 3200), "dp", scatter_dimension=0, tiled=True)
            grads["d", i] = dot(act, d, 0, 0).astype(BF16)
            if not i:
                early, grads["g", 0], grads["d", 0] = lax.optimization_barrier((early, grads["g", 0], grads["d", 0]))
                new["g", 1] = update("g", 1, early[0])
                block, d_up = lax.optimization_barrier((new["g", 1][0], d_up))
                full["g", 1] = lax.all_gather(block, "dp", axis=0, tiled=True)
            grads["u", i] = dot(a, d_up, 0, 0).astype(BF16)
            if i:
                da = dot(d_gate, wg[i], 1, 1).astype(BF16) + dot(d_up, wu[i], 1, 1).astype(BF16)
                da = da.astype(F32)
                wide = h.astype(F32)
                inner = jnp.mean(da * wide, -1, keepdims=True)
                d = d + (scale * da - wide * (scale**3 * inner)).astype(BF16)
        units = [("u", 1), ("d", 1), ("g", 0), ("u", 0), ("d", 0)]
        kinds = tuple(k for k, _ in units)
        summed = dict(zip(units, reduce_scatter([by_chips(grads[u], u[0]) for u in units], kinds, 0)))
        for kind, i in units:
            g = summed[kind, i]
            if kind == "d":
                g = lax.dynamic_slice_in_dim(g, core * 100, 100, 0)
            new[kind, i] = update(kind, i, g)
        mine = jnp.stack([new["d", i][0] for i in range(layers)])
        other = lax.ppermute(mine, "dp", [(k, k + 1 - 2 * (k % 2)) for k in range(32)])
        first = core == 0
        whole = jnp.concatenate([jnp.where(first, mine, other), jnp.where(first, other, mine)], 1)
        part = lax.dynamic_slice_in_dim(whole, core * 512, 512, 2)
        blocks = [part[i] if kind == "d" else new[kind, i][0] for kind, i in units]
        for (kind, i), t in zip(units, all_gather(blocks, kinds, 1)):
            full[kind, i] = t.reshape(old[kind][0].shape[1:])
        outs = [jnp.stack([full[k, i] for i in range(layers)]) for k in "gud"]
        for which in (1, 2):
            outs += [jnp.stack([new[k, i][which] for i in range(layers)]) for k in "gud"]
        return tuple(outs)

    seq, whole, rows = P(("rep", "dp")), P(), P(None, "dp")
    return jax.shard_map(
        local,
        mesh=mesh,
        in_specs=(seq, seq, whole, whole, whole) + (rows,) * 6,
        out_specs=(P("rep"),) * 3 + (P("rep", "dp"),) * 6,
        check_vma=False,
    )
```

```python
import functools

import jax
import jax.numpy as jnp
from jax import lax
from jax.experimental import pallas as pl
from jax.experimental.pallas import tpu as pltpu
from jax.sharding import PartitionSpec as P

F32 = jnp.float32
BF16 = jnp.bfloat16
MESH = pl.DeviceIdType.MESH
WEIGHT = (16, 8, 4, 2, 1)
X, Y, Z1, Z0, CORE = range(5)
ORDERS = ((X, Y, Z0, Z1), (Y, X, Z0, Z1), (Z0, Z1, X, Y))
COLUMNS = ((0, 1280), (1280, 1280), (2560, 640))
ROWS = ((0, 80), (80, 80), (160, 40))
ROWWISE, COLWISE = (32, 3200), (200, 512)
KINDS = ("d", "g", "u")


def dot(a, b, ca, cb):
    return lax.dot_general(a, b, (((ca,), (cb,)), ((), ())), preferred_element_type=F32)


def norm(h):
    wide = h.astype(F32)
    scale = lax.rsqrt(jnp.mean(wide**2, -1, keepdims=True) + 1e-6)
    return (wide * scale).astype(BF16), scale


def adamw(w, m, v, g):
    m = 0.9 * m + 0.1 * g
    v = 0.95 * v + 0.05 * g * g
    step = m * lax.rsqrt(v + 1e-8) + 0.1 * w
    return (w - 0.02 * step).astype(BF16), m, v


def half_of(kind):
    return COLWISE if kind == "d" else ROWWISE


def part_of(kind, color):
    rows, columns = half_of(kind)
    if kind == "d":
        at, n = ROWS[color]
        return (pl.ds(at, n), slice(None)), (n, columns)
    at, n = COLUMNS[color]
    return (slice(None), pl.ds(at, n)), (rows, n)


def place():
    me = lax.axis_index("dp")
    bits = tuple(lax.rem(lax.div(me, w), 2) for w in WEIGHT)
    partners = tuple(me + (1 - 2 * b) * w for b, w in zip(bits, WEIGHT))
    return bits, partners


def greet(partners):
    barrier = pltpu.get_barrier_semaphore()
    for p in partners:
        pl.semaphore_signal(barrier, inc=1, device_id={"dp": p}, device_id_type=MESH)
    pl.semaphore_wait(barrier, len(partners))


def remote(src, dst, send, recv, to):
    return pltpu.make_async_remote_copy(src_ref=src, dst_ref=dst, send_sem=send, recv_sem=recv, device_id={"dp": to}, device_id_type=MESH)


def free_of(index):
    return [i for i in range(4) if index[i] is None]


def for_blocks(index, body):
    free = free_of(index)

    def one(n, _):
        at = list(index)
        for k, i in enumerate(free):
            at[i] = lax.rem(lax.div(n, 2 ** (len(free) - 1 - k)), 2)
        body(tuple(at))
        return 0

    lax.fori_loop(0, 2 ** len(free), one, 0)


def window(index):
    return tuple(slice(None) if i is None else i for i in index)


REDUCED = (("g", 1), ("u", 1), ("d", 1), ("d", 0), ("g", 0), ("u", 0))
ROUND = (0, 1, 2, 3, 5, 6)
SLOT = (0, 1, 2, 3, 0, 1)
SLOT_KINDS = ("g", "u", "d", "d")
COMPUTED = (1, 4, 5)
WIDE = 640
TILES = {0: range(0, 5), 1: range(5, 7), 2: range(7, 9), 3: range(9, 11), 4: range(11, 13), 5: range(13, 15)}


def reduce_kernel(*refs):
    n = len(REDUCED)
    kinds = [k for k, _ in REDUCED]
    given, refs = refs[:3], refs[3:]
    lefts, rights, refs = refs[:2], refs[2:5], refs[5:]
    outs, products, refs = refs[:n], refs[n : n + 3], refs[n + 3 :]
    totals, firsts, refs = refs[:4], refs[4:8], refs[8:]
    gots, refs = [refs[12 * i : 12 * i + 12] for i in range(4)], refs[48:]
    lasts, refs = {2: refs[0], 3: refs[1]}, refs[2:]
    lhs, rhs, tile, send, recv, local, free, lhs_sem, rhs_sem, tile_sem = refs
    grads = {0: given[0], 2: given[1], 3: given[2], 1: products[0], 4: products[1], 5: products[2]}
    bits, partners = place()
    core = bits[CORE]

    def load_lhs(layer):
        return pltpu.make_async_copy(lefts[layer], lhs, lhs_sem)

    def load_rhs(j):
        columns = pl.ds(j % 5 * WIDE, WIDE)
        return pltpu.make_async_copy(rights[j // 5].at[:, columns], rhs.at[j % 2], rhs_sem.at[j % 2])

    def store(j):
        columns = pl.ds(j % 5 * WIDE, WIDE)
        out = products[j // 5].at[:, :, :, :, :, :, columns]
        return pltpu.make_async_copy(tile.at[j % 2], out, tile_sem.at[j % 2])

    load_lhs(1).start()
    load_rhs(0).start()
    greet(partners)

    def halves(u, which):
        if kinds[u] == "d":
            return grads[u].at[:, :, :, :, :, pl.ds(pl.multiple_of(which * 512, 512), 512)]
        return grads[u].at[:, :, :, :, which]

    started, waits, told = {}, {u: [] for u in range(n)}, set()

    def may_write(u, dim):
        if u >= 4 and (u, dim) not in told:
            told.add((u, dim))
            pl.semaphore_wait(free.at[u - 4, dim], 1)

    def begin(u):
        may_write(u, CORE)
        copy = remote(halves(u, 1 - core), firsts[SLOT[u]], send.at[u, 12], recv.at[u, 12], partners[CORE])
        copy.start()
        own = pltpu.make_async_copy(halves(u, core), totals[SLOT[u]], local.at[u])
        own.start()
        started[u] = (copy, own)

    for u in (0, 2, 3):
        begin(u)

    state = {(u, color): [None] * 4 for u in range(n) for color in range(3)}
    flying = {}

    def total(u, color, at, steps):
        where = (*at, *part_of(kinds[u], color)[0])
        value = totals[SLOT[u]][where].astype(F32) + firsts[SLOT[u]][where].astype(F32)
        for s in range(steps):
            rest = tuple(at[i] for i in range(4) if i not in ORDERS[color][: s + 1])
            got = gots[SLOT[u]][color * 4 + s]
            value += (got[rest] if rest else got[...]).astype(F32)
        return value.astype(BF16)

    def launch(u, color, s):
        dim = ORDERS[color][s]
        part, _ = part_of(kinds[u], color)
        index = list(state[u, color])
        index[dim] = 1 - bits[dim]
        k = color * 4 + s

        def ready(at):
            totals[SLOT[u]][(*at, *part)] = total(u, color, at, s)

        for_blocks(index, ready)
        may_write(u, dim)
        copy = remote(totals[SLOT[u]].at[(*window(index), *part)], gots[SLOT[u]][k], send.at[u, k], recv.at[u, k], partners[dim])
        copy.start()
        flying[u, color] = copy
        index[dim] = bits[dim]
        state[u, color] = index

    def step(u, s):
        if s == 0:
            copy, own = started[u]
            own.wait()
            copy.wait_recv()
            waits[u].append(copy)
            for color in range(3):
                launch(u, color, 0)
            return
        for color in range(3):
            copy = flying[u, color]
            copy.wait_recv()
            waits[u].append(copy)
            if s < 4:
                launch(u, color, s)
                continue
            (rows, columns), _ = part_of(kinds[u], color)
            if kinds[u] == "d":
                lasts[u][rows, pl.ds(pl.multiple_of(core * 512, 512), 512)] = total(u, color, bits[:4], 4)
            else:
                outs[u][rows, columns] = total(u, color, bits[:4], 4)
        if s == 4:
            if kinds[u] == "d":
                columns = (slice(None), pl.ds(pl.multiple_of(core * 512, 512), 512))
                copy = remote(lasts[u].at[columns], lasts[u].at[columns], send.at[u, 13], recv.at[u, 13], partners[CORE])
                copy.start()
                flying[u] = copy
            elif u < 2:
                for dim, p in enumerate(partners):
                    pl.semaphore_signal(free.at[u, dim], inc=1, device_id={"dp": p}, device_id_type=MESH)
                for copy in waits.pop(u):
                    copy.wait_send()

    def product(j):
        load_rhs(j).wait()
        if j + 1 < 15:
            load_rhs(j + 1).start()
        if j in (0, 5):
            load_lhs(1 if j == 0 else 0).wait()
        if j % 5 >= 2:
            store(j - 2).wait()

        def rows(i, _):
            left = lhs[pl.ds(pl.multiple_of(i * 256, 256), 256), :]
            out = jnp.dot(left, rhs[j % 2], preferred_element_type=F32).astype(BF16)
            tile[j % 2, lax.div(i, 2), lax.rem(i, 2)] = out.reshape(2, 2, 2, 32, WIDE)
            return 0

        lax.fori_loop(0, 4, rows, 0)
        store(j).start()
        if j == 4:
            load_lhs(0).start()
        if j % 5 == 4:
            store(j - 1).wait()
            store(j).wait()

    for t in range(11):
        steps = [(u, t - ROUND[u]) for u in reversed(range(n)) if 0 <= t - ROUND[u] <= 4]
        tiles = list(TILES.get(t, ()))
        while steps or tiles:
            if steps:
                step(*steps.pop(0))
            for _ in range(max(1, -(-len(tiles) // (len(steps) + 1)))):
                if tiles:
                    product(tiles.pop(0))
        if t in (0, 4, 5):
            begin({0: 1, 4: 4, 5: 5}[t])
    for u in (2, 3):
        copy = flying[u]
        copy.wait_recv()
        waits[u].append(copy)
        outs[u][...] = lasts[u][...]
    for u in waits:
        for copy in waits[u]:
            copy.wait_send()


def reduce_scatter(given, lefts, rights):
    blocks = lambda shape: pltpu.VMEM((2, 2, 2, 2, *shape), BF16)
    scratch = [blocks(half_of(k)) for k in SLOT_KINDS] * 2
    for k in SLOT_KINDS:
        for color in range(3):
            for s in range(4):
                scratch.append(pltpu.VMEM((2,) * (3 - s) + part_of(k, color)[1], BF16))
    scratch += [pltpu.VMEM((200, 1024), BF16)] * 2
    scratch += [pltpu.VMEM((1024, 2048), BF16), pltpu.VMEM((2, 2048, WIDE), BF16), pltpu.VMEM((2, 2, 2, 2, 2, 2, 32, WIDE), BF16)]
    dma = pltpu.SemaphoreType.DMA
    scratch += [dma((6, 14)), dma((6, 14)), dma((6,)), pltpu.SemaphoreType.REGULAR((2, 5)), dma, dma((2,)), dma((2,))]
    hbm, vmem = pl.BlockSpec(memory_space=pltpu.HBM), pl.BlockSpec(memory_space=pltpu.VMEM)
    sums = [jax.ShapeDtypeStruct((200, 1024) if k == "d" else (32, 3200), BF16) for k, _ in REDUCED]
    products = [jax.ShapeDtypeStruct((2, 2, 2, 2, 2, 32, 3200), BF16)] * 3
    return pl.pallas_call(
        reduce_kernel,
        out_shape=sums + products,
        in_specs=[hbm] * 8,
        out_specs=[vmem] * 6 + [hbm] * 3,
        scratch_shapes=scratch,
        compiler_params=pltpu.CompilerParams(collective_id=0, has_side_effects=True, vmem_limit_bytes=63 * 2**20),
        name="reduce",
    )(*given, *lefts, *rights)[:6]


def gather_kernel(kinds, *refs):
    n = len(kinds)
    blocks, outs, (send, recv, local) = refs[:n], refs[n : 2 * n], refs[2 * n :]
    bits, partners = place()
    core = bits[CORE]
    greet(partners)

    def at(u, index, color):
        (rows, columns), _ = part_of(kinds[u], color)
        out = outs[u]
        if kinds[u] == "d":
            return out.at[(*window(index), rows, pl.ds(pl.multiple_of(core * 512, 512), 512))]
        return out.at[(*window(index), core, rows, columns)]

    sent = []
    flying = {}
    state = {}

    def across(u, color, src, index, k):
        dst = at(u, index, color)
        copy = remote(dst if src is None else src, dst, send.at[u, 9 * color + k], recv.at[u, 9 * color + k], partners[CORE])
        copy.start()
        sent.append((copy, True))

    def launch(u, color, s, src=None):
        dim = ORDERS[color][3 - s]
        dst = at(u, state[u, color], color)
        copy = remote(dst if src is None else src, dst, send.at[u, 9 * color + s], recv.at[u, 9 * color + s], partners[dim])
        copy.start()
        flying[u, color] = copy

    for t in range(n + 4):
        for u in reversed(range(n)):
            s = t - u
            if s == 0:
                for color in range(3):
                    state[u, color] = list(bits[:4])
                    (rows, columns), _ = part_of(kinds[u], color)
                    src = blocks[u].at[rows, columns]
                    launch(u, color, 0, src)
                    across(u, color, src, state[u, color], 4)
                    own = pltpu.make_async_copy(src, at(u, state[u, color], color), local.at[u, color])
                    own.start()
                    flying["own", u, color] = own
            elif 0 < s <= 4:
                for color in range(3):
                    copy = flying[u, color]
                    copy.wait_recv()
                    sent.append((copy, False))
                    if s == 1:
                        flying["own", u, color].wait()
                    dim = ORDERS[color][4 - s]
                    fresh = list(state[u, color])
                    fresh[dim] = 1 - bits[dim]
                    state[u, color][dim] = None
                    if s < 4:
                        launch(u, color, s)
                    across(u, color, None, fresh, 4 + s)
    for copy, from_core in sent:
        copy.wait_send()
        if from_core:
            copy.wait_recv()


def all_gather(blocks, kinds, collective_id):
    n = len(kinds)
    shapes = [(2, 2, 2, 2, 200, 1024) if k == "d" else (2, 2, 2, 2, 2, 32, 3200) for k in kinds]
    return pl.pallas_call(
        functools.partial(gather_kernel, kinds),
        out_shape=[jax.ShapeDtypeStruct(s, BF16) for s in shapes],
        in_specs=[pl.BlockSpec(memory_space=pltpu.VMEM)] * n,
        out_specs=[pl.BlockSpec(memory_space=pltpu.HBM)] * n,
        scratch_shapes=[pltpu.SemaphoreType.DMA((n, 27)), pltpu.SemaphoreType.DMA((n, 27)), pltpu.SemaphoreType.DMA((n, 3))],
        compiler_params=pltpu.CompilerParams(collective_id=collective_id, has_side_effects=True),
        name=f"gather_{collective_id}",
    )(*blocks)


def solution(mesh):
    def local(x, dy, wg, wu, wd, mg, mu, md, vg, vu, vd):
        x, dy = x[0], dy[0]
        me = lax.axis_index("dp")
        core = lax.rem(me, 2)
        layers = wg.shape[0]
        old = {"g": (wg, mg, vg), "u": (wu, mu, vu), "d": (wd, md, vd)}

        h = x
        saved = []
        for i in range(layers):
            a, scale = norm(h)
            gate = dot(a, wg[i], 1, 0)
            up = dot(a, wu[i], 1, 0)
            act = (jax.nn.silu(gate) * up).astype(BF16)
            saved.append((h, a, scale, gate, up, act))
            if i + 1 < layers:
                h = h + dot(act, wd[i], 1, 0).astype(BF16)
        def rows_of(t, kind):
            rows = old[kind][1].shape[1]
            return lax.dynamic_slice_in_dim(t, me * rows, rows, 0)

        def update(kind, i, g):
            w, m, v = (t[i] for t in old[kind])
            return adamw(rows_of(w, kind).astype(F32), m, v, g.astype(F32))

        def by_chips(t, kind):
            return t.reshape(2, 2, 2, 2, 200, 1024) if kind == "d" else t.reshape(2, 2, 2, 2, 2, 32, 3200)

        d = dy
        grads, new, full = {}, {}, {}
        lefts, rights = {}, {}
        for i in reversed(range(layers)):
            h, a, scale, gate, up, act = saved[i]
            d_act = dot(d, wd[i], 1, 1).astype(BF16).astype(F32)
            sig = jax.nn.sigmoid(gate)
            d_up = (d_act * (gate * sig)).astype(BF16)
            d_gate = (d_act * up * (sig * (1 + gate * (1 - sig)))).astype(BF16)
            lefts[i] = a.T
            rights["g", i], rights["u", i] = d_gate, d_up
            if i:
                grads["g", i] = dot(a, d_gate, 0, 0).astype(BF16)
            grads["d", i] = dot(act, d, 0, 0).astype(BF16)
            if i:
                da = dot(d_gate, wg[i], 1, 1).astype(BF16) + dot(d_up, wu[i], 1, 1).astype(BF16)
                da = da.astype(F32)
                wide = h.astype(F32)
                inner = jnp.mean(da * wide, -1, keepdims=True)
                d = d + (scale * da - wide * (scale**3 * inner)).astype(BF16)
        units = REDUCED
        kinds = tuple(k for k, _ in units)
        given = [by_chips(grads[u], u[0]) for u in (units[0], units[2], units[3])]
        summed = dict(zip(units, reduce_scatter(given, [lefts[0], lefts[1]], [rights[units[u]] for u in COMPUTED])))
        for kind, i in units:
            g = summed[kind, i]
            if kind == "d":
                g = lax.dynamic_slice_in_dim(g, core * 100, 100, 0)
            new[kind, i] = update(kind, i, g)
        mine = jnp.stack([new["d", i][0] for i in range(layers)])
        other = lax.ppermute(mine, "dp", [(k, k + 1 - 2 * (k % 2)) for k in range(32)])
        first = core == 0
        whole = jnp.concatenate([jnp.where(first, mine, other), jnp.where(first, other, mine)], 1)
        part = lax.dynamic_slice_in_dim(whole, core * 512, 512, 2)
        blocks = [part[i] if kind == "d" else new[kind, i][0] for kind, i in units]
        for (kind, i), t in zip(units, all_gather(blocks, kinds, 1)):
            full[kind, i] = t.reshape(old[kind][0].shape[1:])
        outs = [jnp.stack([full[k, i] for i in range(layers)]) for k in "gud"]
        for which in (1, 2):
            outs += [jnp.stack([new[k, i][which] for i in range(layers)]) for k in "gud"]
        return tuple(outs)

    seq, whole, rows = P(("rep", "dp")), P(), P(None, "dp")
    return jax.shard_map(
        local,
        mesh=mesh,
        in_specs=(seq, seq, whole, whole, whole) + (rows,) * 6,
        out_specs=(P("rep"),) * 3 + (P("rep", "dp"),) * 6,
        check_vma=False,
    )
```

```python
import functools

import jax
import jax.numpy as jnp
from jax import lax
from jax.experimental import pallas as pl
from jax.experimental.pallas import tpu as pltpu
from jax.sharding import PartitionSpec as P

F32 = jnp.float32
BF16 = jnp.bfloat16
MESH = pl.DeviceIdType.MESH
WEIGHT = (16, 8, 4, 2, 1)
X, Y, Z1, Z0, CORE = range(5)
ORDERS = ((X, Y, Z0, Z1), (Y, X, Z0, Z1), (Z0, Z1, X, Y))


def order_of(unit, color):
    order = ORDERS[color]
    return (*order[:2], order[3], order[2]) if color == 2 and unit % 2 else order


COLUMNS = ((0, 1280), (1280, 1280), (2560, 640))
ROWS = ((0, 80), (80, 80), (160, 40))
ROWWISE, COLWISE = (32, 3200), (200, 512)
KINDS = ("d", "g", "u")


def dot(a, b, ca, cb):
    return lax.dot_general(a, b, (((ca,), (cb,)), ((), ())), preferred_element_type=F32)


def norm(h):
    wide = h.astype(F32)
    scale = lax.rsqrt(jnp.mean(wide**2, -1, keepdims=True) + 1e-6)
    return (wide * scale).astype(BF16), scale


def adamw(w, m, v, g):
    m = 0.9 * m + 0.1 * g
    v = 0.95 * v + 0.05 * g * g
    step = m * lax.rsqrt(v + 1e-8) + 0.1 * w
    return (w - 0.02 * step).astype(BF16), m, v


def half_of(kind):
    return COLWISE if kind == "d" else ROWWISE


def part_of(kind, color):
    rows, columns = half_of(kind)
    if kind == "d":
        at, n = ROWS[color]
        return (pl.ds(at, n), slice(None)), (n, columns)
    at, n = COLUMNS[color]
    return (slice(None), pl.ds(at, n)), (rows, n)


def place():
    me = lax.axis_index("dp")
    bits = tuple(lax.rem(lax.div(me, w), 2) for w in WEIGHT)
    partners = tuple(me + (1 - 2 * b) * w for b, w in zip(bits, WEIGHT))
    return bits, partners


def greet(partners):
    barrier = pltpu.get_barrier_semaphore()
    for p in partners:
        pl.semaphore_signal(barrier, inc=1, device_id={"dp": p}, device_id_type=MESH)
    pl.semaphore_wait(barrier, len(partners))


def remote(src, dst, send, recv, to):
    return pltpu.make_async_remote_copy(src_ref=src, dst_ref=dst, send_sem=send, recv_sem=recv, device_id={"dp": to}, device_id_type=MESH)


def free_of(index):
    return [i for i in range(4) if index[i] is None]


def for_blocks(index, body):
    free = free_of(index)

    def one(n, _):
        at = list(index)
        for k, i in enumerate(free):
            at[i] = lax.rem(lax.div(n, 2 ** (len(free) - 1 - k)), 2)
        body(tuple(at))
        return 0

    lax.fori_loop(0, 2 ** len(free), one, 0)


def window(index):
    return tuple(slice(None) if i is None else i for i in index)


REDUCED = (("g", 1), ("u", 1), ("d", 1), ("d", 0), ("g", 0), ("u", 0))
ROUND = (0, 1, 2, 3, 5, 6)
SLOT = (0, 1, 2, 3, 0, 1)
SLOT_KINDS = ("g", "u", "d", "d")
COMPUTED = (1, 4, 5)
WIDE = 640
TILES = {0: range(0, 5), 1: range(5, 8), 2: range(8, 10), 3: range(10, 12), 4: range(12, 15)}


def reduce_kernel(*refs):
    n = len(REDUCED)
    kinds = [k for k, _ in REDUCED]
    given, refs = refs[:3], refs[3:]
    lefts, rights, refs = refs[:2], refs[2:5], refs[5:]
    outs, products, refs = refs[:n], refs[n : n + 3], refs[n + 3 :]
    totals, firsts, refs = refs[:4], refs[4:8], refs[8:]
    gots, refs = [refs[12 * i : 12 * i + 12] for i in range(4)], refs[48:]
    lasts, refs = {2: refs[0], 3: refs[1]}, refs[2:]
    lhs, rhs, tile, send, recv, local, free, lhs_sem, rhs_sem, tile_sem = refs
    grads = {0: given[0], 2: given[1], 3: given[2], 1: products[0], 4: products[1], 5: products[2]}
    bits, partners = place()
    core = bits[CORE]

    def load_lhs(layer):
        return pltpu.make_async_copy(lefts[layer], lhs, lhs_sem)

    def load_rhs(j):
        columns = pl.ds(j % 5 * WIDE, WIDE)
        return pltpu.make_async_copy(rights[j // 5].at[:, columns], rhs.at[j % 2], rhs_sem.at[j % 2])

    def store(j):
        columns = pl.ds(j % 5 * WIDE, WIDE)
        out = products[j // 5].at[:, :, :, :, :, :, columns]
        return pltpu.make_async_copy(tile.at[j % 2], out, tile_sem.at[j % 2])

    load_lhs(1).start()
    load_rhs(0).start()
    greet(partners)

    def halves(u, which):
        if kinds[u] == "d":
            return grads[u].at[:, :, :, :, :, pl.ds(pl.multiple_of(which * 512, 512), 512)]
        return grads[u].at[:, :, :, :, which]

    started, waits, told = {}, {u: [] for u in range(n)}, set()

    def may_write(u, dim):
        if u >= 4 and (u, dim) not in told:
            told.add((u, dim))
            pl.semaphore_wait(free.at[u - 4, dim], 1)

    def begin(u):
        may_write(u, CORE)
        copy = remote(halves(u, 1 - core), firsts[SLOT[u]], send.at[u, 12], recv.at[u, 12], partners[CORE])
        copy.start()
        own = pltpu.make_async_copy(halves(u, core), totals[SLOT[u]], local.at[u])
        own.start()
        started[u] = (copy, own)

    for u in (0, 2, 3):
        begin(u)

    state = {(u, color): [None] * 4 for u in range(n) for color in range(3)}
    flying = {}

    def total(u, color, at, steps):
        where = (*at, *part_of(kinds[u], color)[0])
        value = totals[SLOT[u]][where].astype(F32) + firsts[SLOT[u]][where].astype(F32)
        for s in range(steps):
            rest = tuple(at[i] for i in range(4) if i not in order_of(u, color)[: s + 1])
            got = gots[SLOT[u]][color * 4 + s]
            value += (got[rest] if rest else got[...]).astype(F32)
        return value.astype(BF16)

    def launch(u, color, s):
        dim = order_of(u, color)[s]
        part, _ = part_of(kinds[u], color)
        index = list(state[u, color])
        index[dim] = 1 - bits[dim]
        k = color * 4 + s

        def ready(at):
            totals[SLOT[u]][(*at, *part)] = total(u, color, at, s)

        for_blocks(index, ready)
        may_write(u, dim)
        copy = remote(totals[SLOT[u]].at[(*window(index), *part)], gots[SLOT[u]][k], send.at[u, k], recv.at[u, k], partners[dim])
        copy.start()
        flying[u, color] = copy
        index[dim] = bits[dim]
        state[u, color] = index

    def step(u, s):
        if s == 0:
            copy, own = started[u]
            own.wait()
            copy.wait_recv()
            waits[u].append(copy)
            for color in range(3):
                launch(u, color, 0)
            return
        for color in range(3):
            copy = flying[u, color]
            copy.wait_recv()
            waits[u].append(copy)
            if s < 4:
                launch(u, color, s)
                continue
            (rows, columns), _ = part_of(kinds[u], color)
            if kinds[u] == "d":
                lasts[u][rows, pl.ds(pl.multiple_of(core * 512, 512), 512)] = total(u, color, bits[:4], 4)
            else:
                outs[u][rows, columns] = total(u, color, bits[:4], 4)
        if s == 4:
            if kinds[u] == "d":
                columns = (slice(None), pl.ds(pl.multiple_of(core * 512, 512), 512))
                copy = remote(lasts[u].at[columns], lasts[u].at[columns], send.at[u, 13], recv.at[u, 13], partners[CORE])
                copy.start()
                flying[u] = copy
            elif u < 2:
                for dim, p in enumerate(partners):
                    pl.semaphore_signal(free.at[u, dim], inc=1, device_id={"dp": p}, device_id_type=MESH)
                for copy in waits.pop(u):
                    copy.wait_send()

    def product(j):
        load_rhs(j).wait()
        if j + 1 < 15:
            load_rhs(j + 1).start()
        if j in (0, 5):
            load_lhs(1 if j == 0 else 0).wait()
        if j % 5 >= 2:
            store(j - 2).wait()

        def rows(i, _):
            left = lhs[pl.ds(pl.multiple_of(i * 256, 256), 256), :]
            out = jnp.dot(left, rhs[j % 2], preferred_element_type=F32).astype(BF16)
            tile[j % 2, lax.div(i, 2), lax.rem(i, 2)] = out.reshape(2, 2, 2, 32, WIDE)
            return 0

        lax.fori_loop(0, 4, rows, 0)
        store(j).start()
        if j == 4:
            load_lhs(0).start()
        if j % 5 == 4:
            store(j - 1).wait()
            store(j).wait()

    for t in range(11):
        steps = [(u, t - ROUND[u]) for u in reversed(range(n)) if 0 <= t - ROUND[u] <= 4]
        if t in (4, 5):
            steps.remove((t - 4, 4))
            steps.insert(t - 4, (t - 4, 4))
        tiles = list(TILES.get(t, ()))
        taken = 0
        while steps or tiles:
            if steps:
                step(*steps.pop(0))
                taken += 1
            if t in (4, 5) and taken == t - 2 and t not in started:
                begin(t)
            for _ in range(max(1, -(-len(tiles) // (len(steps) + 1)))):
                if tiles:
                    product(tiles.pop(0))
        if t == 0:
            begin(1)
    for u in (2, 3):
        copy = flying[u]
        copy.wait_recv()
        waits[u].append(copy)
        outs[u][...] = lasts[u][...]
    for u in waits:
        for copy in waits[u]:
            copy.wait_send()


def reduce_scatter(given, lefts, rights):
    blocks = lambda shape: pltpu.VMEM((2, 2, 2, 2, *shape), BF16)
    scratch = [blocks(half_of(k)) for k in SLOT_KINDS] * 2
    for k in SLOT_KINDS:
        for color in range(3):
            for s in range(4):
                scratch.append(pltpu.VMEM((2,) * (3 - s) + part_of(k, color)[1], BF16))
    scratch += [pltpu.VMEM((200, 1024), BF16)] * 2
    scratch += [pltpu.VMEM((1024, 2048), BF16), pltpu.VMEM((2, 2048, WIDE), BF16), pltpu.VMEM((2, 2, 2, 2, 2, 2, 32, WIDE), BF16)]
    dma = pltpu.SemaphoreType.DMA
    scratch += [dma((6, 14)), dma((6, 14)), dma((6,)), pltpu.SemaphoreType.REGULAR((2, 5)), dma, dma((2,)), dma((2,))]
    hbm, vmem = pl.BlockSpec(memory_space=pltpu.HBM), pl.BlockSpec(memory_space=pltpu.VMEM)
    sums = [jax.ShapeDtypeStruct((200, 1024) if k == "d" else (32, 3200), BF16) for k, _ in REDUCED]
    products = [jax.ShapeDtypeStruct((2, 2, 2, 2, 2, 32, 3200), BF16)] * 3
    return pl.pallas_call(
        reduce_kernel,
        out_shape=sums + products,
        in_specs=[hbm] * 8,
        out_specs=[vmem] * 6 + [hbm] * 3,
        scratch_shapes=scratch,
        compiler_params=pltpu.CompilerParams(collective_id=0, has_side_effects=True, vmem_limit_bytes=63 * 2**20),
        name="reduce",
    )(*given, *lefts, *rights)[:6]


def gather_kernel(kinds, *refs):
    n = len(kinds)
    blocks, outs, (send, recv, local) = refs[:n], refs[n : 2 * n], refs[2 * n :]
    bits, partners = place()
    core = bits[CORE]
    greet(partners)

    def at(u, index, color):
        (rows, columns), _ = part_of(kinds[u], color)
        out = outs[u]
        if kinds[u] == "d":
            return out.at[(*window(index), rows, pl.ds(pl.multiple_of(core * 512, 512), 512))]
        return out.at[(*window(index), core, rows, columns)]

    sent = []
    flying = {}
    state = {}

    def across(u, color, src, index, k):
        dst = at(u, index, color)
        copy = remote(dst if src is None else src, dst, send.at[u, 9 * color + k], recv.at[u, 9 * color + k], partners[CORE])
        copy.start()
        sent.append((copy, True))

    def launch(u, color, s, src=None):
        dim = order_of(u, color)[3 - s]
        dst = at(u, state[u, color], color)
        copy = remote(dst if src is None else src, dst, send.at[u, 9 * color + s], recv.at[u, 9 * color + s], partners[dim])
        copy.start()
        flying[u, color] = copy

    for t in range(n + 4):
        for u in reversed(range(n)):
            s = t - u
            if s == 0:
                for color in range(3):
                    state[u, color] = list(bits[:4])
                    (rows, columns), _ = part_of(kinds[u], color)
                    src = blocks[u].at[rows, columns]
                    launch(u, color, 0, src)
                    across(u, color, src, state[u, color], 4)
                    own = pltpu.make_async_copy(src, at(u, state[u, color], color), local.at[u, color])
                    own.start()
                    flying["own", u, color] = own
            elif 0 < s <= 4:
                for color in range(3):
                    copy = flying[u, color]
                    copy.wait_recv()
                    sent.append((copy, False))
                    if s == 1:
                        flying["own", u, color].wait()
                    dim = order_of(u, color)[4 - s]
                    fresh = list(state[u, color])
                    fresh[dim] = 1 - bits[dim]
                    state[u, color][dim] = None
                    if s < 4:
                        launch(u, color, s)
                    across(u, color, None, fresh, 4 + s)
    for copy, from_core in sent:
        copy.wait_send()
        if from_core:
            copy.wait_recv()


def all_gather(blocks, kinds, collective_id):
    n = len(kinds)
    shapes = [(2, 2, 2, 2, 200, 1024) if k == "d" else (2, 2, 2, 2, 2, 32, 3200) for k in kinds]
    return pl.pallas_call(
        functools.partial(gather_kernel, kinds),
        out_shape=[jax.ShapeDtypeStruct(s, BF16) for s in shapes],
        in_specs=[pl.BlockSpec(memory_space=pltpu.VMEM)] * n,
        out_specs=[pl.BlockSpec(memory_space=pltpu.HBM)] * n,
        scratch_shapes=[pltpu.SemaphoreType.DMA((n, 27)), pltpu.SemaphoreType.DMA((n, 27)), pltpu.SemaphoreType.DMA((n, 3))],
        compiler_params=pltpu.CompilerParams(collective_id=collective_id, has_side_effects=True),
        name=f"gather_{collective_id}",
    )(*blocks)


def solution(mesh):
    def local(x, dy, wg, wu, wd, mg, mu, md, vg, vu, vd):
        x, dy = x[0], dy[0]
        me = lax.axis_index("dp")
        core = lax.rem(me, 2)
        layers = wg.shape[0]
        old = {"g": (wg, mg, vg), "u": (wu, mu, vu), "d": (wd, md, vd)}

        h = x
        saved = []
        for i in range(layers):
            a, scale = norm(h)
            gate = dot(a, wg[i], 1, 0)
            up = dot(a, wu[i], 1, 0)
            act = (jax.nn.silu(gate) * up).astype(BF16)
            saved.append((h, a, scale, gate, up, act))
            if i + 1 < layers:
                h = h + dot(act, wd[i], 1, 0).astype(BF16)
        def by_chips(t, kind):
            return t.reshape(2, 2, 2, 2, 200, 1024) if kind == "d" else t.reshape(2, 2, 2, 2, 2, 32, 3200)

        d = dy
        grads, new, full = {}, {}, {}
        lefts, rights = {}, {}
        for i in reversed(range(layers)):
            h, a, scale, gate, up, act = saved[i]
            d_act = dot(d, wd[i], 1, 1).astype(BF16).astype(F32)
            sig = jax.nn.sigmoid(gate)
            d_up = (d_act * (gate * sig)).astype(BF16)
            d_gate = (d_act * up * (sig * (1 + gate * (1 - sig)))).astype(BF16)
            lefts[i] = a.T
            rights["g", i], rights["u", i] = d_gate, d_up
            if i:
                grads["g", i] = dot(a, d_gate, 0, 0).astype(BF16)
            grads["d", i] = dot(act, d, 0, 0).astype(BF16)
            if i:
                da = dot(d_gate, wg[i], 1, 1).astype(BF16) + dot(d_up, wu[i], 1, 1).astype(BF16)
                da = da.astype(F32)
                wide = h.astype(F32)
                inner = jnp.mean(da * wide, -1, keepdims=True)
                d = d + (scale * da - wide * (scale**3 * inner)).astype(BF16)
        units = REDUCED
        kinds = tuple(k for k, _ in units)
        given = [by_chips(grads[u], u[0]) for u in (units[0], units[2], units[3])]
        summed = dict(zip(units, reduce_scatter(given, [lefts[0], lefts[1]], [rights[units[u]] for u in COMPUTED])))
        for kind in KINDS:
            w, m, v = old[kind]
            rows = m.shape[1]
            g = jnp.stack([summed[kind, i] for i in range(layers)])
            if kind == "d":
                g = lax.dynamic_slice_in_dim(g, core * rows, rows, 1)
            mine = lax.dynamic_slice_in_dim(w, me * rows, rows, 1)
            new[kind] = adamw(mine.astype(F32), m, v, g.astype(F32))
        mine = new["d"][0]
        other = lax.ppermute(mine, "dp", [(k, k + 1 - 2 * (k % 2)) for k in range(32)])
        first = core == 0
        whole = jnp.concatenate([jnp.where(first, mine, other), jnp.where(first, other, mine)], 1)
        part = lax.dynamic_slice_in_dim(whole, core * 512, 512, 2)
        blocks = [part[i] if kind == "d" else new[kind][0][i] for kind, i in units]
        for (kind, i), t in zip(units, all_gather(blocks, kinds, 1)):
            full[kind, i] = t.reshape(old[kind][0].shape[1:])
        outs = [jnp.stack([full[k, i] for i in range(layers)]) for k in "gud"]
        for which in (1, 2):
            outs += [new[k][which] for k in "gud"]
        return tuple(outs)

    seq, whole, rows = P(("rep", "dp")), P(), P(None, "dp")
    return jax.shard_map(
        local,
        mesh=mesh,
        in_specs=(seq, seq, whole, whole, whole) + (rows,) * 6,
        out_specs=(P("rep"),) * 3 + (P("rep", "dp"),) * 6,
        check_vma=False,
    )
```
